32 devices in a mesh: scen: 2 (over y), row: 4 (over z), col: 2 (over x), layer: 2 (over core).
Axes of the slice: x: 2, y: 2, z: 4, core: 2. Of those that a mesh axis runs over, the one named last changes fastest.
Arguments:
- current: float32 [2, 1024, 2048], P('layer', ('scen', 'row'), 'col'), parts along dimension 1, may hold values from 0.5 to 10
- node_class: int32 [2, 1024, 2048], P('layer', ('scen', 'row'), 'col'), parts along dimension 1, may hold values from 0 to 7
- class_conductance: float32 [2, 8], P('layer'), may hold values from 0.5 to 4
- pad_mask: int32 [2, 1024, 2048], P('layer', ('scen', 'row'), 'col'), parts along dimension 1, may hold values 0 or 1
- via_mask: int32 [1024, 2048], P(('scen', 'row'), 'col'), parts along dimension 0, may hold values 0 or 1
Outputs:
- drop: float32 [2, 1024, 2048], P('layer', ('scen', 'row'), 'col'), parts along dimension 1
- residual: float32 [2, 1024, 2048], P('layer', ('scen', 'row'), 'col'), parts along dimension 1
- worst: float32 [2, 1024, 2048], P('layer', ('scen', 'row'), 'col'), parts along dimension 1
The draws below stay inside these ranges and needn't reach their ends.
There are 2 independent parts, one for each index of `scen`. The reference program is written for one: setup_inputs(seed, part) draws one part's arguments, and reference() takes and returns one part's arrays. A program takes and returns all parts, laid end to end along the dimension named above; an argument that names none is the same for every part. Nothing has to cross between parts.
All inputs are finite; a program needn't handle non-finite values. No bound on the sum of `pad_mask` or of `via_mask` on one device may be relied on, other than what follows from the above.
Results may differ from the reference program's by a relative error of at most 0.0003.
Values sent between devices are 32-bit elements; how exact they have to be, the bound alone decides.
A program may use at most 64 MiB of HBM per device.

```python
import math
import jax
import jax.numpy as jnp

CLASSES = 8
ITERS = 2
NX = 512
NY = 2048
LAYERS = 2


def with_ends(entries, stream_key, smallest, high):
    spot = [jax.random.randint(jax.random.fold_in(stream_key, axis), (), 0, length) for axis, length in enumerate(entries.shape)]
    longest = entries.shape.index(max(entries.shape))
    next_to = spot[:longest] + [(spot[longest] + 1) % entries.shape[longest]] + spot[longest + 1:]
    return entries.at[tuple(spot)].set(smallest).at[tuple(next_to)].set(high)


def shard_levels(rng, shape, shards, low, high):
    def one(position, shards_of):
        steps = jax.random.uniform(jax.random.fold_in(jax.random.fold_in(rng, 6), position), (shards_of,), jnp.float32, low / len(shards), high / len(shards))
        return jnp.repeat(jnp.exp(steps), shape[position] // shards_of).reshape((-1,) + (1,) * (len(shape) - position - 1))

    gain = one(*shards[0])
    for cut in shards[1:]:
        gain = gain * one(*cut)
    return gain


def setup_inputs(seed: int = 0, part: int = 0) -> dict:
    streams_of = jax.random.split(jax.random.key(seed), 6)
    own_keys = jax.random.split(jax.random.fold_in(streams_of[5], part), 6)
    return {
        "current": jnp.clip(jnp.exp(math.log(10.0) - 2.9957323 * jax.random.uniform(own_keys[0], (LAYERS, NX, NY), jnp.float32) ** shard_levels(own_keys[0], (LAYERS, NX, NY), ((0, 2), (1, 4), (2, 2)), -0.2, 0.2)), 0.5, 10.0),
        "node_class": with_ends(jax.random.randint(own_keys[1], (LAYERS, NX, NY), 0, CLASSES), jax.random.fold_in(own_keys[1], 1), 0, CLASSES - 1).astype(jnp.int32),
        "class_conductance": jnp.clip(jnp.exp(math.log(4.0) - 2.0794415 * jax.random.uniform(streams_of[2], (LAYERS, CLASSES), jnp.float32) ** shard_levels(streams_of[2], (LAYERS, CLASSES), ((0, 2),), -0.2, 0.2)), 0.5, 4.0),
        "pad_mask": with_ends((jax.random.randint(own_keys[3], (LAYERS, NX, NY), 0, 16) < 1).astype(jnp.int32), jax.random.fold_in(own_keys[3], 1), 0, 1),
        "via_mask": with_ends((jax.random.randint(own_keys[4], (NX, NY), 0, 2) < 1).astype(jnp.int32), jax.random.fold_in(own_keys[4], 1), 0, 1),
    }


via_conductance = 2.0
pad_conductance = 4.0
leakage = 0.05


def lookup(node_class, class_conductance):
    cond = jnp.zeros(node_class.shape, jnp.float32)
    for klass in range(class_conductance.shape[1]):
        cond = cond + jnp.where(node_class == klass, class_conductance[:, klass][:, None, None], jnp.float32(0.0))
    return cond


def edge_terms(cond):
    padded = jnp.pad(cond, ((0, 0), (1, 1), (1, 1)))
    beside_all = (padded[:, :-2, 1:-1], padded[:, 2:, 1:-1], padded[:, 1:-1, :-2], padded[:, 1:-1, 2:])
    return tuple(jnp.where(other > 0.0, 0.5 * (cond + other), jnp.float32(0.0)) for other in beside_all)


def apply_grid(values, edges, diagonal, coupling):
    padded = jnp.pad(values, ((0, 0), (1, 1), (1, 1)))
    beside = edges[0] * padded[:, :-2, 1:-1] + edges[1] * padded[:, 2:, 1:-1]
    beside = beside + edges[2] * padded[:, 1:-1, :-2] + edges[3] * padded[:, 1:-1, 2:]
    return diagonal * values - beside - coupling * values[::-1]


def reference(current, node_class, class_conductance, pad_mask, via_mask):
    cond = lookup(node_class, class_conductance)
    edges = edge_terms(cond)
    coupling = via_conductance * via_mask.astype(jnp.float32)
    diagonal = edges[0] + edges[1] + edges[2] + edges[3] + coupling + pad_conductance * pad_mask.astype(jnp.float32) + leakage
    drop_field = jnp.zeros_like(current)
    resid = current
    precond = resid / diagonal
    direction = precond
    energy_now = jnp.sum(resid * precond)
    worst_field = drop_field
    for iteration in range(ITERS):
        image = apply_grid(direction, edges, diagonal, coupling)
        step_size = energy_now / jnp.sum(direction * image)
        drop_field = drop_field + step_size * direction
        resid = resid - step_size * image
        worst_field = drop_field if iteration == 0 else jnp.maximum(worst_field, drop_field)
        if iteration + 1 < ITERS:
            precond = resid / diagonal
            energy_next = jnp.sum(resid * precond)
            direction = precond + (energy_next / energy_now) * direction
            energy_now = energy_next
    return drop_field, resid, worst_field
```

```python
import functools

import jax
import jax.numpy as jnp
from jax import lax
from jax.experimental import pallas as pl
from jax.experimental.pallas import tpu as pltpu
from jax.sharding import PartitionSpec as P

MESH = pl.DeviceIdType.MESH
PAD = 8
SLAB = 8
via_conductance = 2.0
pad_conductance = 4.0
leakage = 0.05


def fold(x):
    parts = [x[:, k : k + 128] for k in range(0, x.shape[1], 128)]
    while len(parts) > 1:
        half = len(parts) // 2
        parts = [parts[k] + parts[k + half] for k in range(half)] + parts[2 * half :]
    return parts[0]


def kernel(sizes, cur_hbm, cls_hbm, table, pad_hbm, via_hbm, drop_hbm, res_hbm, worst_hbm,
           cur, cls, pad, via, cond, edge, inv, zed, zedq, wed, yed, yedq, ued, out,
           row_out, row_in, col_out, col_in, side, gather,
           load_sem, edge_send, edge_recv, layer_send, layer_recv, sum_send, sum_recv, store_sem):
    rows, cols, layers = sizes
    height, width = cur.shape
    me_r, me_c, me_l = lax.axis_index("row"), lax.axis_index("col"), lax.axis_index("layer")
    others = rows * cols * layers - 1
    slabs = height // SLAB

    def peer(k):
        r = lax.rem(me_r + k // (cols * layers), rows)
        c = lax.rem(me_c + lax.rem(k // layers, cols), cols)
        l = lax.rem(me_l + lax.rem(k, layers), layers)
        return {"row": r, "col": c, "layer": l}

    def each_peer(body):
        if others < 32:
            for k in range(1, others + 1):
                body(k)
        else:
            def step(k, carry):
                body(k)
                return carry
            lax.fori_loop(1, others + 1, step, 0)

    loads = [
        pltpu.make_async_copy(src, dst, load_sem.at[k])
        for k, (src, dst) in enumerate(
            ((cls_hbm.at[0], cls), (via_hbm, via), (pad_hbm.at[0], pad), (cur_hbm.at[0], cur))
        )
    ]
    for load in loads:
        load.start()

    barrier = pltpu.get_barrier_semaphore()
    each_peer(lambda k: pl.semaphore_signal(barrier, inc=1, device_id=peer(k), device_id_type=MESH))

    present = (me_r > 0, me_r < rows - 1, me_c > 0, me_c < cols - 1)
    exists = (rows > 1, rows > 1, cols > 1, cols > 1)
    target = ({"row": me_r - 1}, {"row": me_r + 1}, {"col": me_c - 1}, {"col": me_c + 1})

    def border(rnd, way):
        src = row_out if way < 2 else col_out
        dst = row_in if way < 2 else col_in
        return pltpu.make_async_remote_copy(
            src_ref=src.at[rnd, way % 2],
            dst_ref=dst.at[rnd, 1 - way % 2],
            send_sem=edge_send.at[rnd, way],
            recv_sem=edge_recv.at[rnd, way ^ 1],
            device_id=target[way],
            device_id_type=MESH,
        )

    def arrival(rnd, way):
        buf = row_in if way < 2 else col_in
        return pltpu.make_async_copy(
            buf.at[rnd, way % 2], buf.at[rnd, way % 2], edge_recv.at[rnd, way]
        )

    def send_borders(rnd, field):
        row_out[rnd, 0] = field[PAD : PAD + 1, :]
        row_out[rnd, 1] = field[PAD + height - 1 : PAD + height, :]
        for way in (0, 1):
            if exists[way]:
                pl.when(present[way])(lambda way=way: border(rnd, way).start())
        col_out[rnd, 0] = jnp.transpose(field[PAD : PAD + height, 0:128])[0:1, :]
        col_out[rnd, 1] = jnp.transpose(field[PAD : PAD + height, width - 128 : width])[127:128, :]
        for way in (2, 3):
            if exists[way]:
                pl.when(present[way])(lambda way=way: border(rnd, way).start())

    def take_borders(rnd, field):
        for way in range(4):
            if exists[way]:
                pl.when(present[way])(lambda way=way: arrival(rnd, way).wait())
        field[PAD - 1 : PAD, :] = row_in[rnd, 0]
        field[PAD + height : PAD + height + 1, :] = row_in[rnd, 1]
        for k in range(2):
            side[k] = jnp.transpose(jnp.broadcast_to(col_in[rnd, k], (128, height)))

    def clear(rnd):
        for way in range(4):
            buf = row_in if way < 2 else col_in
            def zero(buf=buf, way=way):
                buf[rnd, way % 2] = jnp.zeros(buf.shape[2:], jnp.float32)
            if exists[way]:
                pl.when(jnp.logical_not(present[way]))(zero)
            else:
                zero()

    for rnd in range(3):
        clear(rnd)

    lane = lax.broadcasted_iota(jnp.int32, (SLAB, 128), 1)

    def around(field, s):
        lo = PAD + s * SLAB
        here = field[lo : lo + SLAB, :]
        north = field[lo - 1 : lo + SLAB - 1, :]
        south = field[lo + 1 : lo + SLAB + 1, :]
        left, right = pltpu.roll(here, 1, 1), pltpu.roll(here, width - 1, 1)
        at = slice(s * SLAB, (s + 1) * SLAB)
        west = jnp.concatenate(
            [jnp.where(lane == 0, side[0, at, :], left[:, :128]), left[:, 128:]], axis=1)
        east = jnp.concatenate(
            [right[:, :-128], jnp.where(lane == 127, side[1, at, :], right[:, -128:])], axis=1)
        return here, (north, south, west, east)

    def to_partner(rnd, s):
        at = pl.ds(s * chunk, chunk)
        src = (zed, yed)[rnd].at[pl.ds(PAD + s * chunk, chunk)]
        return pltpu.make_async_remote_copy(
            src_ref=src, dst_ref=(zedq, yedq)[rnd].at[at],
            send_sem=layer_send.at[rnd, s], recv_sem=layer_recv.at[rnd, s],
            device_id={"layer": 1 - me_l}, device_id_type=MESH)

    chunks = layer_send.shape[1]
    chunk = height // chunks

    loads[0].wait()
    for s in range(slabs):
        at = slice(s * SLAB, (s + 1) * SLAB)
        klass = cls[at, :]
        value = jnp.full(klass.shape, table[0, 0], jnp.float32)
        for k in range(1, table.shape[1]):
            value = jnp.where(klass == k, table[0, k], value)
        cond[PAD + s * SLAB : PAD + (s + 1) * SLAB, :] = value

    pl.semaphore_wait(barrier, others)
    send_borders(0, cond)
    for load in loads[1:]:
        load.wait()
    take_borders(0, cond)

    for s in range(slabs):
        at = slice(s * SLAB, (s + 1) * SLAB)
        here, beside = around(cond, s)
        diagonal = via_conductance * via[at, :].astype(jnp.float32)
        diagonal = diagonal + pad_conductance * pad[at, :].astype(jnp.float32) + leakage
        for k in range(4):
            value = jnp.where(beside[k] > 0.0, 0.5 * (here + beside[k]), 0.0)
            edge[k, at, :] = value
            diagonal = diagonal + value
        recip = 1.0 / diagonal
        inv[at, :] = recip
        zed[PAD + s * SLAB : PAD + (s + 1) * SLAB, :] = cur[at, :] * recip
        if (s + 1) * SLAB % chunk == 0:
            to_partner(0, (s + 1) * SLAB // chunk - 1).start()
    send_borders(1, zed)

    def image(rnd, field, other, base, s):
        at = slice(s * SLAB, (s + 1) * SLAB)
        if s * SLAB % chunk == 0:
            to_partner(rnd, s * SLAB // chunk).wait_recv()
        here, beside = around(field, s)
        total = edge[0, at, :] * beside[0] + edge[1, at, :] * beside[1]
        total = total + (edge[2, at, :] * beside[2] + edge[3, at, :] * beside[3])
        cross = via_conductance * via[at, :].astype(jnp.float32) * other[at, :]
        return here, base - total - cross

    take_borders(1, zed)
    gamma = delta = eps = jnp.zeros((SLAB, 128), jnp.float32)
    for s in range(slabs):
        at = slice(s * SLAB, (s + 1) * SLAB)
        here, w = image(0, zed, zedq, cur[at, :], s)
        y = w * inv[at, :]
        wed[at, :] = w
        yed[PAD + s * SLAB : PAD + (s + 1) * SLAB, :] = y
        gamma = gamma + fold(cur[at, :] * here)
        delta = delta + fold(w * here)
        eps = eps + fold(w * y)
        if (s + 1) * SLAB % chunk == 0:
            to_partner(1, (s + 1) * SLAB // chunk - 1).start()
    send_borders(2, yed)

    eps_all = jnp.sum(eps, keepdims=True)
    delta_all = jnp.sum(delta, keepdims=True)
    a_d = jnp.where(eps_all > 0.0, delta_all / jnp.where(eps_all > 0.0, eps_all, 1.0), 0.0)

    take_borders(2, yed)
    s0 = s1 = t0 = t1 = t2 = jnp.zeros((SLAB, 128), jnp.float32)
    for s in range(slabs):
        at = slice(s * SLAB, (s + 1) * SLAB)
        w = wed[at, :]
        y, u = image(1, yed, yedq, w, s)
        ued[at, :] = u
        r1 = cur[at, :] - a_d * w
        z1 = zed[PAD + s * SLAB : PAD + (s + 1) * SLAB, :] - a_d * y
        w1 = w - a_d * u
        s0 = s0 + fold(r1 * z1)
        s1 = s1 + fold(w * z1)
        t0 = t0 + fold(z1 * w1)
        t1 = t1 + fold(z1 * u + y * w1)
        t2 = t2 + fold(y * u)

    packet = jnp.zeros((SLAB, 128), jnp.float32)
    for k, value in enumerate((gamma, delta, s0, s1, eps, t0, t1, t2)):
        packet = packet + jnp.where(lane == k, jnp.sum(value, axis=1, keepdims=True), 0.0)
    packet = jnp.sum(packet, axis=0, keepdims=True)
    packet = jnp.where(lane[0:1] == 8, a_d, packet)
    gather[0] = packet

    def share(k):
        return pltpu.make_async_remote_copy(
            src_ref=gather.at[0], dst_ref=gather.at[k], send_sem=sum_send, recv_sem=sum_recv,
            device_id=peer(k), device_id_type=MESH)

    each_peer(lambda k: share(k).start())
    everyone = gather.at[pl.ds(1, others)]
    pltpu.make_async_copy(everyone, everyone, sum_recv).wait()

    table_in = gather[...].reshape(others + 1, 128)
    lanes = lax.broadcasted_iota(jnp.int32, table_in.shape, 1)
    g, d, s0, s1, s2, t0, t1, t2, a_ds = (
        jnp.sum(jnp.where(lanes == k, table_in, 0.0), axis=1, keepdims=True) for k in range(9)
    )
    energy = jnp.sum(g, axis=0, keepdims=True)
    step = energy / jnp.sum(d, axis=0, keepdims=True)
    away = step - a_ds
    energy_next = jnp.sum(s0 - 2.0 * away * s1 + away * away * s2, axis=0, keepdims=True)
    curve = jnp.sum(t0 - away * t1 + away * away * t2, axis=0, keepdims=True)
    ratio = energy_next / energy
    step_next = energy_next / (curve - ratio * energy_next / step)

    stores = []
    for s in range(slabs):
        at = slice(s * SLAB, (s + 1) * SLAB)
        z = zed[PAD + s * SLAB : PAD + (s + 1) * SLAB, :]
        y = yed[PAD + s * SLAB : PAD + (s + 1) * SLAB, :]
        w = wed[at, :]
        first = step * z
        drop = first + step_next * ((z - step * y) + ratio * z)
        out[0, at, :] = drop
        out[1, at, :] = (cur[at, :] - step * w) - step_next * ((w - step * ued[at, :]) + ratio * w)
        out[2, at, :] = jnp.maximum(first, drop)
        if (s + 1) * SLAB % chunk == 0:
            c = (s + 1) * SLAB // chunk - 1
            for k, dst in enumerate((drop_hbm, res_hbm, worst_hbm)):
                store = pltpu.make_async_copy(
                    out.at[k, pl.ds(c * chunk, chunk)], dst.at[0, pl.ds(c * chunk, chunk)],
                    store_sem.at[k, c])
                store.start()
                stores.append(store)

    for rnd in range(3):
        for way in range(4):
            if exists[way]:
                pl.when(present[way])(lambda rnd=rnd, way=way: border(rnd, way).wait_send())
    for rnd in range(2):
        for c in range(chunks):
            to_partner(rnd, c).wait_send()
    pltpu.make_async_copy(everyone, everyone, sum_send).wait()
    for store in stores:
        store.wait()


def local(sizes, current, node_class, class_conductance, pad_mask, via_mask):
    _, height, width = current.shape
    f32 = jnp.float32
    chunks = 4
    full = lambda kind=f32: pltpu.VMEM((height, width), kind)
    tall = pltpu.VMEM((height + 2 * PAD, width), f32)
    anywhere = pl.BlockSpec(memory_space=pl.ANY)
    dma = pltpu.SemaphoreType.DMA
    return pl.pallas_call(
        functools.partial(kernel, sizes),
        out_shape=[jax.ShapeDtypeStruct(current.shape, f32)] * 3,
        in_specs=[anywhere, anywhere, pl.BlockSpec(memory_space=pltpu.SMEM), anywhere, anywhere],
        out_specs=[anywhere] * 3,
        scratch_shapes=[
            full(), full(jnp.int32), full(jnp.int32), full(jnp.int32),
            tall, pltpu.VMEM((4, height, width), f32), full(),
            tall, full(), full(), tall, full(), full(), pltpu.VMEM((3, height, width), f32),
            pltpu.VMEM((3, 2, 1, width), f32), pltpu.VMEM((3, 2, 1, width), f32),
            pltpu.VMEM((3, 2, 1, height), f32), pltpu.VMEM((3, 2, 1, height), f32),
            pltpu.VMEM((2, height, 128), f32),
            pltpu.VMEM((sizes[0] * sizes[1] * sizes[2], 1, 128), f32),
            dma((4,)), dma((3, 4)), dma((3, 4)), dma((2, chunks)), dma((2, chunks)),
            dma, dma, dma((3, chunks)),
        ],
        compiler_params=pltpu.CompilerParams(collective_id=0, has_side_effects=True),
    )(current, node_class, class_conductance, pad_mask, via_mask)


def solution(mesh):
    field = P("layer", ("scen", "row"), "col")
    sizes = tuple(mesh.shape[name] for name in ("row", "col", "layer"))
    return jax.shard_map(
        functools.partial(local, sizes),
        mesh=mesh,
        in_specs=(field, field, P("layer", None), field, P(("scen", "row"), "col")),
        out_specs=(field, field, field),
        check_vma=False,
    )
```

```python
import functools

import jax
import jax.numpy as jnp
from jax import lax
from jax.experimental import pallas as pl
from jax.experimental.pallas import tpu as pltpu
from jax.sharding import PartitionSpec as P

MESH = pl.DeviceIdType.MESH
PAD = 8
SLAB = 8
via_conductance = 2.0
pad_conductance = 4.0
leakage = 0.05


def fold(x):
    parts = [x[:, k : k + 128] for k in range(0, x.shape[1], 128)]
    while len(parts) > 1:
        half = len(parts) // 2
        parts = [parts[k] + parts[k + half] for k in range(half)] + parts[2 * half :]
    return parts[0]


def kernel(sizes, cur_hbm, cls_hbm, table, pad_hbm, via_hbm, cur, zed, wed, yed, ued, scal,
           cls, pad, via, cond, edge, inv, zedq, yedq,
           row_out, row_in, col_out, col_in, side, gather,
           load_sem, edge_send, edge_recv, layer_send, layer_recv, sum_send, sum_recv):
    rows, cols, layers = sizes
    height, width = cur.shape
    me_r, me_c, me_l = lax.axis_index("row"), lax.axis_index("col"), lax.axis_index("layer")
    others = rows * cols * layers - 1
    slabs = height // SLAB

    def peer(k):
        r = lax.rem(me_r + k // (cols * layers), rows)
        c = lax.rem(me_c + lax.rem(k // layers, cols), cols)
        l = lax.rem(me_l + lax.rem(k, layers), layers)
        return {"row": r, "col": c, "layer": l}

    def each_peer(body):
        if others < 32:
            for k in range(1, others + 1):
                body(k)
        else:
            def step(k, carry):
                body(k)
                return carry
            lax.fori_loop(1, others + 1, step, 0)

    loads = [
        pltpu.make_async_copy(src, dst, load_sem.at[k])
        for k, (src, dst) in enumerate(
            ((cls_hbm.at[0], cls), (via_hbm, via), (pad_hbm.at[0], pad), (cur_hbm.at[0], cur))
        )
    ]
    for load in loads:
        load.start()

    barrier = pltpu.get_barrier_semaphore()
    each_peer(lambda k: pl.semaphore_signal(barrier, inc=1, device_id=peer(k), device_id_type=MESH))

    present = (me_r > 0, me_r < rows - 1, me_c > 0, me_c < cols - 1)
    exists = (rows > 1, rows > 1, cols > 1, cols > 1)
    target = ({"row": me_r - 1}, {"row": me_r + 1}, {"col": me_c - 1}, {"col": me_c + 1})

    def border(rnd, way):
        src = row_out if way < 2 else col_out
        dst = row_in if way < 2 else col_in
        return pltpu.make_async_remote_copy(
            src_ref=src.at[rnd, way % 2],
            dst_ref=dst.at[rnd, 1 - way % 2],
            send_sem=edge_send.at[rnd, way],
            recv_sem=edge_recv.at[rnd, way ^ 1],
            device_id=target[way],
            device_id_type=MESH,
        )

    def arrival(rnd, way):
        buf = row_in if way < 2 else col_in
        return pltpu.make_async_copy(
            buf.at[rnd, way % 2], buf.at[rnd, way % 2], edge_recv.at[rnd, way]
        )

    def send_borders(rnd, field):
        row_out[rnd, 0] = field[PAD : PAD + 1, :]
        row_out[rnd, 1] = field[PAD + height - 1 : PAD + height, :]
        for way in (0, 1):
            if exists[way]:
                pl.when(present[way])(lambda way=way: border(rnd, way).start())
        col_out[rnd, 0] = jnp.transpose(field[PAD : PAD + height, 0:128])[0:1, :]
        col_out[rnd, 1] = jnp.transpose(field[PAD : PAD + height, width - 128 : width])[127:128, :]
        for way in (2, 3):
            if exists[way]:
                pl.when(present[way])(lambda way=way: border(rnd, way).start())

    def take_borders(rnd, field):
        for way in range(4):
            if exists[way]:
                pl.when(present[way])(lambda way=way: arrival(rnd, way).wait())
        field[PAD - 1 : PAD, :] = row_in[rnd, 0]
        field[PAD + height : PAD + height + 1, :] = row_in[rnd, 1]
        for k in range(2):
            side[k] = jnp.transpose(jnp.broadcast_to(col_in[rnd, k], (128, height)))

    def clear(rnd):
        for way in range(4):
            buf = row_in if way < 2 else col_in
            def zero(buf=buf, way=way):
                buf[rnd, way % 2] = jnp.zeros(buf.shape[2:], jnp.float32)
            if exists[way]:
                pl.when(jnp.logical_not(present[way]))(zero)
            else:
                zero()

    for rnd in range(3):
        clear(rnd)

    lane = lax.broadcasted_iota(jnp.int32, (SLAB, 128), 1)

    def around(field, s):
        lo = PAD + s * SLAB
        here = field[lo : lo + SLAB, :]
        north = field[lo - 1 : lo + SLAB - 1, :]
        south = field[lo + 1 : lo + SLAB + 1, :]
        left, right = pltpu.roll(here, 1, 1), pltpu.roll(here, width - 1, 1)
        at = slice(s * SLAB, (s + 1) * SLAB)
        west = jnp.concatenate(
            [jnp.where(lane == 0, side[0, at, :], left[:, :128]), left[:, 128:]], axis=1)
        east = jnp.concatenate(
            [right[:, :-128], jnp.where(lane == 127, side[1, at, :], right[:, -128:])], axis=1)
        return here, (north, south, west, east)

    def to_partner(rnd, s):
        at = pl.ds(s * chunk, chunk)
        src = (zed, yed)[rnd].at[pl.ds(PAD + s * chunk, chunk)]
        return pltpu.make_async_remote_copy(
            src_ref=src, dst_ref=(zedq, yedq)[rnd].at[at],
            send_sem=layer_send.at[rnd, s], recv_sem=layer_recv.at[rnd, s],
            device_id={"layer": 1 - me_l}, device_id_type=MESH)

    chunks = layer_send.shape[1]
    chunk = height // chunks

    loads[0].wait()
    for s in range(slabs):
        at = slice(s * SLAB, (s + 1) * SLAB)
        klass = cls[at, :]
        value = jnp.full(klass.shape, table[0, 0], jnp.float32)
        for k in range(1, table.shape[1]):
            value = jnp.where(klass == k, table[0, k], value)
        cond[PAD + s * SLAB : PAD + (s + 1) * SLAB, :] = value

    pl.semaphore_wait(barrier, others)
    send_borders(0, cond)
    for load in loads[1:]:
        load.wait()
    take_borders(0, cond)

    for s in range(slabs):
        at = slice(s * SLAB, (s + 1) * SLAB)
        here, beside = around(cond, s)
        diagonal = via_conductance * via[at, :].astype(jnp.float32)
        diagonal = diagonal + pad_conductance * pad[at, :].astype(jnp.float32) + leakage
        for k in range(4):
            value = jnp.where(beside[k] > 0.0, 0.5 * (here + beside[k]), 0.0)
            edge[k, at, :] = value
            diagonal = diagonal + value
        recip = 1.0 / diagonal
        inv[at, :] = recip
        zed[PAD + s * SLAB : PAD + (s + 1) * SLAB, :] = cur[at, :] * recip
        if (s + 1) * SLAB % chunk == 0:
            to_partner(0, (s + 1) * SLAB // chunk - 1).start()
    send_borders(1, zed)

    def image(rnd, field, other, base, s):
        at = slice(s * SLAB, (s + 1) * SLAB)
        if s * SLAB % chunk == 0:
            to_partner(rnd, s * SLAB // chunk).wait_recv()
        here, beside = around(field, s)
        total = edge[0, at, :] * beside[0] + edge[1, at, :] * beside[1]
        total = total + (edge[2, at, :] * beside[2] + edge[3, at, :] * beside[3])
        cross = via_conductance * via[at, :].astype(jnp.float32) * other[at, :]
        return here, base - total - cross

    take_borders(1, zed)
    gamma = delta = eps = jnp.zeros((SLAB, 128), jnp.float32)
    for s in range(slabs):
        at = slice(s * SLAB, (s + 1) * SLAB)
        here, w = image(0, zed, zedq, cur[at, :], s)
        y = w * inv[at, :]
        wed[at, :] = w
        yed[PAD + s * SLAB : PAD + (s + 1) * SLAB, :] = y
        gamma = gamma + fold(cur[at, :] * here)
        delta = delta + fold(w * here)
        eps = eps + fold(w * y)
        if (s + 1) * SLAB % chunk == 0:
            to_partner(1, (s + 1) * SLAB // chunk - 1).start()
    send_borders(2, yed)

    eps_all = jnp.sum(eps, keepdims=True)
    delta_all = jnp.sum(delta, keepdims=True)
    a_d = jnp.where(eps_all > 0.0, delta_all / jnp.where(eps_all > 0.0, eps_all, 1.0), 0.0)

    take_borders(2, yed)
    s0 = s1 = t0 = t1 = t2 = jnp.zeros((SLAB, 128), jnp.float32)
    for s in range(slabs):
        at = slice(s * SLAB, (s + 1) * SLAB)
        w = wed[at, :]
        y, u = image(1, yed, yedq, w, s)
        ued[at, :] = u
        r1 = cur[at, :] - a_d * w
        z1 = zed[PAD + s * SLAB : PAD + (s + 1) * SLAB, :] - a_d * y
        w1 = w - a_d * u
        s0 = s0 + fold(r1 * z1)
        s1 = s1 + fold(w * z1)
        t0 = t0 + fold(z1 * w1)
        t1 = t1 + fold(z1 * u + y * w1)
        t2 = t2 + fold(y * u)

    packet = jnp.zeros((SLAB, 128), jnp.float32)
    for k, value in enumerate((gamma, delta, s0, s1, eps, t0, t1, t2)):
        packet = packet + jnp.where(lane == k, jnp.sum(value, axis=1, keepdims=True), 0.0)
    packet = jnp.sum(packet, axis=0, keepdims=True)
    packet = jnp.where(lane[0:1] == 8, a_d, packet)
    gather[0] = packet

    def share(k):
        return pltpu.make_async_remote_copy(
            src_ref=gather.at[0], dst_ref=gather.at[k], send_sem=sum_send, recv_sem=sum_recv,
            device_id=peer(k), device_id_type=MESH)

    each_peer(lambda k: share(k).start())
    everyone = gather.at[pl.ds(1, others)]
    pltpu.make_async_copy(everyone, everyone, sum_recv).wait()

    table_in = gather[...].reshape(others + 1, 128)
    lanes = lax.broadcasted_iota(jnp.int32, table_in.shape, 1)
    g, d, s0, s1, s2, t0, t1, t2, a_ds = (
        jnp.sum(jnp.where(lanes == k, table_in, 0.0), axis=1, keepdims=True) for k in range(9)
    )
    energy = jnp.sum(g, axis=0, keepdims=True)
    step = energy / jnp.sum(d, axis=0, keepdims=True)
    away = step - a_ds
    energy_next = jnp.sum(s0 - 2.0 * away * s1 + away * away * s2, axis=0, keepdims=True)
    curve = jnp.sum(t0 - away * t1 + away * away * t2, axis=0, keepdims=True)
    ratio = energy_next / energy
    step_next = energy_next / (curve - ratio * energy_next / step)

    for k, value in enumerate((step, step_next, ratio)):
        scal[k : k + 1, :] = jnp.broadcast_to(value, (1, 128))

    for rnd in range(3):
        for way in range(4):
            if exists[way]:
                pl.when(present[way])(lambda rnd=rnd, way=way: border(rnd, way).wait_send())
    for rnd in range(2):
        for c in range(chunks):
            to_partner(rnd, c).wait_send()
    pltpu.make_async_copy(everyone, everyone, sum_send).wait()


def finish(cur, zed, wed, yed, ued, scal, drop_hbm, res_hbm, worst_hbm, out, store_sem):
    height = cur.shape[0]
    slabs = height // SLAB
    chunks = store_sem.shape[1]
    chunk = height // chunks
    step, step_next, ratio = (scal[k : k + 1, 0:1] for k in range(3))
    stores = []
    for s in range(slabs):
        at = slice(s * SLAB, (s + 1) * SLAB)
        z = zed[PAD + s * SLAB : PAD + (s + 1) * SLAB, :]
        y = yed[PAD + s * SLAB : PAD + (s + 1) * SLAB, :]
        w = wed[at, :]
        first = step * z
        drop = first + step_next * ((z - step * y) + ratio * z)
        out[0, at, :] = drop
        out[1, at, :] = (cur[at, :] - step * w) - step_next * ((w - step * ued[at, :]) + ratio * w)
        out[2, at, :] = jnp.maximum(first, drop)
        if (s + 1) * SLAB % chunk == 0:
            c = (s + 1) * SLAB // chunk - 1
            for k, dst in enumerate((drop_hbm, res_hbm, worst_hbm)):
                store = pltpu.make_async_copy(
                    out.at[k, pl.ds(c * chunk, chunk)], dst.at[0, pl.ds(c * chunk, chunk)],
                    store_sem.at[k, c])
                store.start()
                stores.append(store)

    for store in stores:
        store.wait()


def local(sizes, current, node_class, class_conductance, pad_mask, via_mask):
    _, height, width = current.shape
    f32 = jnp.float32
    chunks = 4
    full = lambda kind=f32: pltpu.VMEM((height, width), kind)
    tall = pltpu.VMEM((height + 2 * PAD, width), f32)
    anywhere = pl.BlockSpec(memory_space=pl.ANY)
    dma = pltpu.SemaphoreType.DMA
    kept = [(height, width), tall.shape, (height, width), tall.shape, (height, width), (8, 128)]
    far = pl.BlockSpec(memory_space=pltpu.HBM)
    inside = pl.BlockSpec(memory_space=pltpu.VMEM)
    fields = pl.pallas_call(
        functools.partial(kernel, sizes),
        out_shape=[pltpu.VMEM(shape, f32) for shape in kept],
        in_specs=[far, far, pl.BlockSpec(memory_space=pltpu.SMEM), far, far],
        out_specs=[inside] * len(kept),
        scratch_shapes=[
            full(jnp.int32), full(jnp.int32), full(jnp.int32),
            tall, pltpu.VMEM((4, height, width), f32), full(), full(), full(),
            pltpu.VMEM((3, 2, 1, width), f32), pltpu.VMEM((3, 2, 1, width), f32),
            pltpu.VMEM((3, 2, 1, height), f32), pltpu.VMEM((3, 2, 1, height), f32),
            pltpu.VMEM((2, height, 128), f32),
            pltpu.VMEM((sizes[0] * sizes[1] * sizes[2], 1, 128), f32),
            dma((4,)), dma((3, 4)), dma((3, 4)), dma((2, chunks)), dma((2, chunks)), dma, dma,
        ],
        compiler_params=pltpu.CompilerParams(
            collective_id=0, has_side_effects=True, vmem_limit_bytes=56 * 2**20),
    )(current, node_class, class_conductance, pad_mask, via_mask)
    return pl.pallas_call(
        finish,
        out_shape=[jax.ShapeDtypeStruct(current.shape, f32)] * 3,
        in_specs=[inside] * len(kept),
        out_specs=[anywhere] * 3,
        scratch_shapes=[pltpu.VMEM((3, height, width), f32), dma((3, chunks))],
        compiler_params=pltpu.CompilerParams(vmem_limit_bytes=8 * 2**20),
    )(*fields)


def solution(mesh):
    field = P("layer", ("scen", "row"), "col")
    sizes = tuple(mesh.shape[name] for name in ("row", "col", "layer"))
    return jax.shard_map(
        functools.partial(local, sizes),
        mesh=mesh,
        in_specs=(field, field, P("layer", None), field, P(("scen", "row"), "col")),
        out_specs=(field, field, field),
        check_vma=False,
    )
```

```python
import functools

import jax
import jax.numpy as jnp
from jax import lax
from jax.experimental import pallas as pl
from jax.experimental.pallas import tpu as pltpu
from jax.sharding import PartitionSpec as P

MESH = pl.DeviceIdType.MESH
PAD = 8
SLAB = 8
via_conductance = 2.0
pad_conductance = 4.0
leakage = 0.05


def fold(x):
    parts = [x[:, k : k + 128] for k in range(0, x.shape[1], 128)]
    while len(parts) > 1:
        half = len(parts) // 2
        parts = [parts[k] + parts[k + half] for k in range(half)] + parts[2 * half :]
    return parts[0]


def kernel(sizes, cur_hbm, cls_hbm, table, pad_hbm, via_hbm, cur, zed, wed, yed, ued, scal,
           cls, pad, via, cond, edge, inv, zedq, yedq,
           row_out, row_in, col_out, col_in, side, gather,
           load_sem, edge_send, edge_recv, layer_send, layer_recv, sum_send, sum_recv):
    rows, cols, layers = sizes
    height, width = cur.shape
    me_r, me_c, me_l = lax.axis_index("row"), lax.axis_index("col"), lax.axis_index("layer")
    others = rows * cols * layers - 1
    slabs = height // SLAB

    def peer(k):
        r = lax.rem(me_r + k // (cols * layers), rows)
        c = lax.rem(me_c + lax.rem(k // layers, cols), cols)
        l = lax.rem(me_l + lax.rem(k, layers), layers)
        return {"row": r, "col": c, "layer": l}

    def each_peer(body):
        if others < 32:
            for k in range(1, others + 1):
                body(k)
        else:
            def step(k, carry):
                body(k)
                return carry
            lax.fori_loop(1, others + 1, step, 0)

    loads = [
        pltpu.make_async_copy(src, dst, load_sem.at[k])
        for k, (src, dst) in enumerate(
            ((cls_hbm.at[0], cls), (via_hbm, via), (pad_hbm.at[0], pad), (cur_hbm.at[0], cur))
        )
    ]
    for load in loads:
        load.start()

    barrier = pltpu.get_barrier_semaphore()
    def greet(k):
        pl.semaphore_signal(barrier, inc=1, device_id=peer(k), device_id_type=MESH)

    if rows <= 4:
        plane = cols * layers
        for k in range(1, plane):
            greet(k)
        for way, row in ((0, me_r - 1), (1, me_r + 1)):
            def beyond(row=row):
                for k in range(plane):
                    c = lax.rem(me_c + k // layers, cols)
                    l = lax.rem(me_l + k % layers, layers)
                    pl.semaphore_signal(barrier, inc=1, device_id={"row": row, "col": c, "layer": l},
                                        device_id_type=MESH)
            if rows > 1:
                pl.when((me_r > 0, me_r < rows - 1)[way])(beyond)
        sides = 1 + (me_r > 0).astype(jnp.int32) + (me_r < rows - 1).astype(jnp.int32)
        greeted = sides * plane - 1
    else:
        each_peer(greet)
        greeted = others

    present = (me_r > 0, me_r < rows - 1, me_c > 0, me_c < cols - 1)
    exists = (rows > 1, rows > 1, cols > 1, cols > 1)
    target = ({"row": me_r - 1}, {"row": me_r + 1}, {"col": me_c - 1}, {"col": me_c + 1})

    def border(rnd, way):
        src = row_out if way < 2 else col_out
        dst = row_in if way < 2 else col_in
        return pltpu.make_async_remote_copy(
            src_ref=src.at[rnd, way % 2],
            dst_ref=dst.at[rnd, 1 - way % 2],
            send_sem=edge_send.at[rnd, way],
            recv_sem=edge_recv.at[rnd, way ^ 1],
            device_id=target[way],
            device_id_type=MESH,
        )

    def arrival(rnd, way):
        buf = row_in if way < 2 else col_in
        return pltpu.make_async_copy(
            buf.at[rnd, way % 2], buf.at[rnd, way % 2], edge_recv.at[rnd, way]
        )

    def send_borders(rnd, field):
        row_out[rnd, 0] = field[PAD : PAD + 1, :]
        row_out[rnd, 1] = field[PAD + height - 1 : PAD + height, :]
        for way in (0, 1):
            if exists[way]:
                pl.when(present[way])(lambda way=way: border(rnd, way).start())
        col_out[rnd, 0] = jnp.transpose(field[PAD : PAD + height, 0:128])[0:1, :]
        col_out[rnd, 1] = jnp.transpose(field[PAD : PAD + height, width - 128 : width])[127:128, :]
        for way in (2, 3):
            if exists[way]:
                pl.when(present[way])(lambda way=way: border(rnd, way).start())

    def take_borders(rnd, field):
        for way in range(4):
            if exists[way]:
                pl.when(present[way])(lambda way=way: arrival(rnd, way).wait())
        field[PAD - 1 : PAD, :] = row_in[rnd, 0]
        field[PAD + height : PAD + height + 1, :] = row_in[rnd, 1]
        for k in range(2):
            side[k] = jnp.transpose(jnp.broadcast_to(col_in[rnd, k], (128, height)))

    def clear(rnd):
        for way in range(4):
            buf = row_in if way < 2 else col_in
            def zero(buf=buf, way=way):
                buf[rnd, way % 2] = jnp.zeros(buf.shape[2:], jnp.float32)
            if exists[way]:
                pl.when(jnp.logical_not(present[way]))(zero)
            else:
                zero()

    for rnd in range(3):
        clear(rnd)

    lane = lax.broadcasted_iota(jnp.int32, (SLAB, 128), 1)

    inner = (128, width - 128)
    middle = [(s, *inner) for s in range(1, slabs - 1)]
    rim = [(0, 0, width), (slabs - 1, 0, width)]
    rim += [(s, lo, hi) for s in range(1, slabs - 1) for lo, hi in ((0, 128), (width - 128, width))]

    def around(field, piece):
        s, lo, hi = piece
        top = PAD + s * SLAB
        at = slice(s * SLAB, (s + 1) * SLAB)
        north = field[top - 1 : top + SLAB - 1, lo:hi]
        south = field[top + 1 : top + SLAB + 1, lo:hi]
        first, last = max(lo - 128, 0), min(hi + 128, width)
        wide = field[top : top + SLAB, first:last]
        here = wide[:, lo - first : hi - first]
        west = pltpu.roll(wide, 1, 1)[:, lo - first : hi - first]
        east = pltpu.roll(wide, last - first - 1, 1)[:, lo - first : hi - first]
        if lo == 0:
            edge_tile = jnp.where(lane == 0, side[0, at, :], west[:, :128])
            west = edge_tile if hi == 128 else jnp.concatenate([edge_tile, west[:, 128:]], axis=1)
        if hi == width:
            edge_tile = jnp.where(lane == 127, side[1, at, :], east[:, -128:])
            east = edge_tile if hi - lo == 128 else jnp.concatenate([east[:, :-128], edge_tile], axis=1)
        return here, (north, south, west, east)

    blocks = (
        (SLAB, height - SLAB, *inner),
        (0, SLAB, 0, width), (height - SLAB, height, 0, width),
        (SLAB, height - SLAB, 0, 128), (SLAB, height - SLAB, width - 128, width),
    )

    def to_partner(rnd, b):
        top, bottom, lo, hi = blocks[b]
        src = (zed, yed)[rnd].at[pl.ds(PAD + top, bottom - top), pl.ds(lo, hi - lo)]
        dst = (zedq, yedq)[rnd].at[pl.ds(top, bottom - top), pl.ds(lo, hi - lo)]
        return pltpu.make_async_remote_copy(
            src_ref=src, dst_ref=dst,
            send_sem=layer_send.at[rnd, b], recv_sem=layer_recv.at[rnd, b],
            device_id={"layer": 1 - me_l}, device_id_type=MESH)

    loads[0].wait()
    for s in range(slabs):
        at = slice(s * SLAB, (s + 1) * SLAB)
        klass = cls[at, :]
        value = jnp.full(klass.shape, table[0, 0], jnp.float32)
        for k in range(1, table.shape[1]):
            value = jnp.where(klass == k, table[0, k], value)
        cond[PAD + s * SLAB : PAD + (s + 1) * SLAB, :] = value

    pl.semaphore_wait(barrier, greeted)
    send_borders(0, cond)
    for load in loads[1:]:
        load.wait()

    def setup(piece):
        s, lo, hi = piece
        at = slice(s * SLAB, (s + 1) * SLAB)
        here, beside = around(cond, piece)
        diagonal = via_conductance * via[at, lo:hi].astype(jnp.float32)
        diagonal = diagonal + pad_conductance * pad[at, lo:hi].astype(jnp.float32) + leakage
        for k in range(4):
            value = jnp.where(beside[k] > 0.0, 0.5 * (here + beside[k]), 0.0)
            edge[k, at, lo:hi] = value
            diagonal = diagonal + value
        recip = 1.0 / diagonal
        inv[at, lo:hi] = recip
        zed[PAD + s * SLAB : PAD + (s + 1) * SLAB, lo:hi] = cur[at, lo:hi] * recip

    def image(field, other, base, piece):
        s, lo, hi = piece
        at = slice(s * SLAB, (s + 1) * SLAB)
        here, beside = around(field, piece)
        total = edge[0, at, lo:hi] * beside[0] + edge[1, at, lo:hi] * beside[1]
        total = total + (edge[2, at, lo:hi] * beside[2] + edge[3, at, lo:hi] * beside[3])
        cross = via_conductance * via[at, lo:hi].astype(jnp.float32) * other[at, lo:hi]
        return here, base - total - cross

    def ahead(sums, piece):
        s, lo, hi = piece
        at = slice(s * SLAB, (s + 1) * SLAB)
        base = cur[at, lo:hi]
        here, w = image(zed, zedq, base, piece)
        y = w * inv[at, lo:hi]
        wed[at, lo:hi] = w
        yed[PAD + s * SLAB : PAD + (s + 1) * SLAB, lo:hi] = y
        terms = (base * here, w * here, w * y)
        return tuple(total + fold(term) for total, term in zip(sums, terms))

    def depart(rnd, field):
        send_borders(rnd + 1, field)
        for b in range(1, len(blocks)):
            to_partner(rnd, b).start()

    def meanwhile(rnd, work, sums):
        to_partner(rnd, 0).wait_recv()
        for piece in middle:
            sums = work(sums, piece)
        return sums

    def arrive(rnd, field, work, sums):
        take_borders(rnd + 1, field)
        for b in range(1, len(blocks)):
            to_partner(rnd, b).wait_recv()
        for piece in rim:
            sums = work(sums, piece)
        return sums

    for piece in middle:
        setup(piece)
    to_partner(0, 0).start()
    take_borders(0, cond)
    for piece in rim:
        setup(piece)

    nothing = jnp.zeros((SLAB, 128), jnp.float32)
    depart(0, zed)
    sums = meanwhile(0, ahead, (nothing,) * 3)
    to_partner(1, 0).start()
    gamma, delta, eps = arrive(0, zed, ahead, sums)
    depart(1, yed)

    eps_all = jnp.sum(eps, keepdims=True)
    delta_all = jnp.sum(delta, keepdims=True)
    a_d = jnp.where(eps_all > 0.0, delta_all / jnp.where(eps_all > 0.0, eps_all, 1.0), 0.0)

    def again(sums, piece):
        s, lo, hi = piece
        at = slice(s * SLAB, (s + 1) * SLAB)
        w = wed[at, lo:hi]
        y, u = image(yed, yedq, w, piece)
        ued[at, lo:hi] = u
        r1 = cur[at, lo:hi] - a_d * w
        z1 = zed[PAD + s * SLAB : PAD + (s + 1) * SLAB, lo:hi] - a_d * y
        w1 = w - a_d * u
        terms = (r1 * z1, w * z1, z1 * w1, z1 * u + y * w1, y * u)
        return tuple(total + fold(term) for total, term in zip(sums, terms))

    sums = meanwhile(1, again, (nothing,) * 5)
    s0, s1, t0, t1, t2 = arrive(1, yed, again, sums)

    packet = jnp.zeros((SLAB, 128), jnp.float32)
    for k, value in enumerate((gamma, delta, s0, s1, eps, t0, t1, t2)):
        packet = packet + jnp.where(lane == k, jnp.sum(value, axis=1, keepdims=True), 0.0)
    packet = jnp.sum(packet, axis=0, keepdims=True)
    packet = jnp.where(lane[0:1] == 8, a_d, packet)
    gather[0] = packet

    def share(k):
        return pltpu.make_async_remote_copy(
            src_ref=gather.at[0], dst_ref=gather.at[k], send_sem=sum_send, recv_sem=sum_recv,
            device_id=peer(k), device_id_type=MESH)

    each_peer(lambda k: share(k).start())
    everyone = gather.at[pl.ds(1, others)]
    pltpu.make_async_copy(everyone, everyone, sum_recv).wait()

    table_in = gather[...].reshape(others + 1, 128)
    lanes = lax.broadcasted_iota(jnp.int32, table_in.shape, 1)
    g, d, s0, s1, s2, t0, t1, t2, a_ds = (
        jnp.sum(jnp.where(lanes == k, table_in, 0.0), axis=1, keepdims=True) for k in range(9)
    )
    energy = jnp.sum(g, axis=0, keepdims=True)
    step = energy / jnp.sum(d, axis=0, keepdims=True)
    away = step - a_ds
    energy_next = jnp.sum(s0 - 2.0 * away * s1 + away * away * s2, axis=0, keepdims=True)
    curve = jnp.sum(t0 - away * t1 + away * away * t2, axis=0, keepdims=True)
    ratio = energy_next / energy
    step_next = energy_next / (curve - ratio * energy_next / step)

    for k, value in enumerate((step, step_next, ratio)):
        scal[k : k + 1, :] = jnp.broadcast_to(value, (1, 128))

    for rnd in range(3):
        for way in range(4):
            if exists[way]:
                pl.when(present[way])(lambda rnd=rnd, way=way: border(rnd, way).wait_send())
    for rnd in range(2):
        for b in range(len(blocks)):
            to_partner(rnd, b).wait_send()
    pltpu.make_async_copy(everyone, everyone, sum_send).wait()


def finish(cur, zed, wed, yed, ued, scal, drop_hbm, res_hbm, worst_hbm, out, store_sem):
    height = cur.shape[0]
    slabs = height // SLAB
    chunks = store_sem.shape[1]
    chunk = height // chunks
    step, step_next, ratio = (scal[k : k + 1, 0:1] for k in range(3))
    stores = []
    for s in range(slabs):
        at = slice(s * SLAB, (s + 1) * SLAB)
        z = zed[PAD + s * SLAB : PAD + (s + 1) * SLAB, :]
        y = yed[PAD + s * SLAB : PAD + (s + 1) * SLAB, :]
        w = wed[at, :]
        first = step * z
        drop = first + step_next * ((z - step * y) + ratio * z)
        out[0, at, :] = drop
        out[1, at, :] = (cur[at, :] - step * w) - step_next * ((w - step * ued[at, :]) + ratio * w)
        out[2, at, :] = jnp.maximum(first, drop)
        if (s + 1) * SLAB % chunk == 0:
            c = (s + 1) * SLAB // chunk - 1
            for k, dst in enumerate((drop_hbm, res_hbm, worst_hbm)):
                store = pltpu.make_async_copy(
                    out.at[k, pl.ds(c * chunk, chunk)], dst.at[0, pl.ds(c * chunk, chunk)],
                    store_sem.at[k, c])
                store.start()
                stores.append(store)

    for store in stores:
        store.wait()


def local(sizes, current, node_class, class_conductance, pad_mask, via_mask):
    _, height, width = current.shape
    f32 = jnp.float32
    chunks = 4
    full = lambda kind=f32: pltpu.VMEM((height, width), kind)
    tall = pltpu.VMEM((height + 2 * PAD, width), f32)
    anywhere = pl.BlockSpec(memory_space=pl.ANY)
    dma = pltpu.SemaphoreType.DMA
    kept = [(height, width), tall.shape, (height, width), tall.shape, (height, width), (8, 128)]
    far = pl.BlockSpec(memory_space=pltpu.HBM)
    inside = pl.BlockSpec(memory_space=pltpu.VMEM)
    fields = pl.pallas_call(
        functools.partial(kernel, sizes),
        out_shape=[pltpu.VMEM(shape, f32) for shape in kept],
        in_specs=[far, far, pl.BlockSpec(memory_space=pltpu.SMEM), far, far],
        out_specs=[inside] * len(kept),
        scratch_shapes=[
            full(jnp.int32), full(jnp.int32), full(jnp.int32),
            tall, pltpu.VMEM((4, height, width), f32), full(), full(), full(),
            pltpu.VMEM((3, 2, 1, width), f32), pltpu.VMEM((3, 2, 1, width), f32),
            pltpu.VMEM((3, 2, 1, height), f32), pltpu.VMEM((3, 2, 1, height), f32),
            pltpu.VMEM((2, height, 128), f32),
            pltpu.VMEM((sizes[0] * sizes[1] * sizes[2], 1, 128), f32),
            dma((4,)), dma((3, 4)), dma((3, 4)), dma((2, 5)), dma((2, 5)), dma, dma,
        ],
        compiler_params=pltpu.CompilerParams(
            collective_id=0, has_side_effects=True, vmem_limit_bytes=56 * 2**20),
    )(current, node_class, class_conductance, pad_mask, via_mask)
    return pl.pallas_call(
        finish,
        out_shape=[jax.ShapeDtypeStruct(current.shape, f32)] * 3,
        in_specs=[inside] * len(kept),
        out_specs=[anywhere] * 3,
        scratch_shapes=[pltpu.VMEM((3, height, width), f32), dma((3, chunks))],
        compiler_params=pltpu.CompilerParams(vmem_limit_bytes=8 * 2**20),
    )(*fields)


def solution(mesh):
    field = P("layer", ("scen", "row"), "col")
    sizes = tuple(mesh.shape[name] for name in ("row", "col", "layer"))
    return jax.shard_map(
        functools.partial(local, sizes),
        mesh=mesh,
        in_specs=(field, field, P("layer", None), field, P(("scen", "row"), "col")),
        out_specs=(field, field, field),
        check_vma=False,
    )
```

```python
import functools

import jax
import jax.numpy as jnp
from jax import lax
from jax.experimental import pallas as pl
from jax.experimental.pallas import tpu as pltpu
from jax.sharding import PartitionSpec as P

MESH = pl.DeviceIdType.MESH
PAD = 8
SLAB = 8
via_conductance = 2.0
pad_conductance = 4.0
leakage = 0.05


def fold(x):
    parts = [x[:, k : k + 128] for k in range(0, x.shape[1], 128)]
    while len(parts) > 1:
        half = len(parts) // 2
        parts = [parts[k] + parts[k + half] for k in range(half)] + parts[2 * half :]
    return parts[0]


def kernel(sizes, cur_hbm, cls_hbm, table, pad_hbm, via_hbm, cur, zed, wed, yed, ued, scal,
           cls, pad, via, cond, edge, inv, zedq, yedq,
           row_out, row_in, col_out, col_in, side, gather,
           load_sem, edge_send, edge_recv, layer_send, layer_recv, sum_send, sum_recv):
    rows, cols, layers = sizes
    height, width = cur.shape
    me_r, me_c, me_l = lax.axis_index("row"), lax.axis_index("col"), lax.axis_index("layer")
    others = rows * cols * layers - 1
    slabs = height // SLAB

    def peer(k):
        r = lax.rem(me_r + k // (cols * layers), rows)
        c = lax.rem(me_c + lax.rem(k // layers, cols), cols)
        l = lax.rem(me_l + lax.rem(k, layers), layers)
        return {"row": r, "col": c, "layer": l}

    def each_peer(body):
        if others < 32:
            for k in range(1, others + 1):
                body(k)
        else:
            def step(k, carry):
                body(k)
                return carry
            lax.fori_loop(1, others + 1, step, 0)

    inner = (128, width - 128)
    middle = [(s, *inner) for s in range(1, slabs - 1)]
    rim = [(0, 0, width), (slabs - 1, 0, width)]
    rim += [(s, lo, hi) for s in range(1, slabs - 1) for lo, hi in ((0, 128), (width - 128, width))]

    blocks = (
        (SLAB, height - SLAB, *inner),
        (0, SLAB, 0, width), (height - SLAB, height, 0, width),
        (SLAB, height - SLAB, 0, 128), (SLAB, height - SLAB, width - 128, width),
    )

    def load_class(b):
        top, bottom, lo, hi = blocks[b]
        return pltpu.make_async_copy(
            cls_hbm.at[0, pl.ds(top, bottom - top), pl.ds(lo, hi - lo)],
            cls.at[pl.ds(top, bottom - top), pl.ds(lo, hi - lo)], load_sem.at[3 + b])

    loads = [
        pltpu.make_async_copy(src, dst, load_sem.at[k])
        for k, (src, dst) in enumerate(
            ((via_hbm, via), (pad_hbm.at[0], pad), (cur_hbm.at[0], cur)))
    ]
    for b in (1, 2, 3, 4, 0):
        load_class(b).start()
    barrier = pltpu.get_barrier_semaphore()
    def greet(k):
        pl.semaphore_signal(barrier, inc=1, device_id=peer(k), device_id_type=MESH)

    if rows + cols <= 6:
        for k in range(1, layers):
            greet(k)
        greeted = layers - 1
        near = (
            ("row", me_r - 1, me_r > 0), ("row", me_r + 1, me_r < rows - 1),
            ("col", me_c - 1, me_c > 0), ("col", me_c + 1, me_c < cols - 1),
        )
        for axis, there, is_there in near:
            def beyond(axis=axis, there=there):
                for k in range(layers):
                    l = lax.rem(me_l + k, layers)
                    pl.semaphore_signal(barrier, inc=1, device_id={axis: there, "layer": l},
                                        device_id_type=MESH)
            if (rows if axis == "row" else cols) > 1:
                pl.when(is_there)(beyond)
                greeted = greeted + layers * is_there.astype(jnp.int32)
    else:
        each_peer(greet)
        greeted = others

    for load in loads:
        load.start()

    present = (me_r > 0, me_r < rows - 1, me_c > 0, me_c < cols - 1)
    exists = (rows > 1, rows > 1, cols > 1, cols > 1)
    target = ({"row": me_r - 1}, {"row": me_r + 1}, {"col": me_c - 1}, {"col": me_c + 1})

    def border(rnd, way):
        src = row_out if way < 2 else col_out
        dst = row_in if way < 2 else col_in
        return pltpu.make_async_remote_copy(
            src_ref=src.at[rnd, way % 2],
            dst_ref=dst.at[rnd, 1 - way % 2],
            send_sem=edge_send.at[rnd, way],
            recv_sem=edge_recv.at[rnd, way ^ 1],
            device_id=target[way],
            device_id_type=MESH,
        )

    def arrival(rnd, way):
        buf = row_in if way < 2 else col_in
        return pltpu.make_async_copy(
            buf.at[rnd, way % 2], buf.at[rnd, way % 2], edge_recv.at[rnd, way]
        )

    def send_borders(rnd, field):
        row_out[rnd, 0] = field[PAD : PAD + 1, :]
        row_out[rnd, 1] = field[PAD + height - 1 : PAD + height, :]
        for way in (0, 1):
            if exists[way]:
                pl.when(present[way])(lambda way=way: border(rnd, way).start())
        col_out[rnd, 0] = jnp.transpose(field[PAD : PAD + height, 0:128])[0:1, :]
        col_out[rnd, 1] = jnp.transpose(field[PAD : PAD + height, width - 128 : width])[127:128, :]
        for way in (2, 3):
            if exists[way]:
                pl.when(present[way])(lambda way=way: border(rnd, way).start())

    def take_borders(rnd, field):
        for way in range(4):
            if exists[way]:
                pl.when(present[way])(lambda way=way: arrival(rnd, way).wait())
        field[PAD - 1 : PAD, :] = row_in[rnd, 0]
        field[PAD + height : PAD + height + 1, :] = row_in[rnd, 1]
        for k in range(2):
            side[k] = jnp.transpose(jnp.broadcast_to(col_in[rnd, k], (128, height)))

    def clear(rnd):
        for way in range(4):
            buf = row_in if way < 2 else col_in
            def zero(buf=buf, way=way):
                buf[rnd, way % 2] = jnp.zeros(buf.shape[2:], jnp.float32)
            if exists[way]:
                pl.when(jnp.logical_not(present[way]))(zero)
            else:
                zero()

    for rnd in range(3):
        clear(rnd)

    lane = lax.broadcasted_iota(jnp.int32, (SLAB, 128), 1)

    def around(field, piece):
        s, lo, hi = piece
        top = PAD + s * SLAB
        at = slice(s * SLAB, (s + 1) * SLAB)
        north = field[top - 1 : top + SLAB - 1, lo:hi]
        south = field[top + 1 : top + SLAB + 1, lo:hi]
        first, last = max(lo - 128, 0), min(hi + 128, width)
        wide = field[top : top + SLAB, first:last]
        here = wide[:, lo - first : hi - first]
        west = pltpu.roll(wide, 1, 1)[:, lo - first : hi - first]
        east = pltpu.roll(wide, last - first - 1, 1)[:, lo - first : hi - first]
        if lo == 0:
            edge_tile = jnp.where(lane == 0, side[0, at, :], west[:, :128])
            west = edge_tile if hi == 128 else jnp.concatenate([edge_tile, west[:, 128:]], axis=1)
        if hi == width:
            edge_tile = jnp.where(lane == 127, side[1, at, :], east[:, -128:])
            east = edge_tile if hi - lo == 128 else jnp.concatenate([east[:, :-128], edge_tile], axis=1)
        return here, (north, south, west, east)

    def to_partner(rnd, b):
        top, bottom, lo, hi = blocks[b]
        src = (zed, yed)[rnd].at[pl.ds(PAD + top, bottom - top), pl.ds(lo, hi - lo)]
        dst = (zedq, yedq)[rnd].at[pl.ds(top, bottom - top), pl.ds(lo, hi - lo)]
        return pltpu.make_async_remote_copy(
            src_ref=src, dst_ref=dst,
            send_sem=layer_send.at[rnd, b], recv_sem=layer_recv.at[rnd, b],
            device_id={"layer": 1 - me_l}, device_id_type=MESH)

    def lookup(piece):
        s, lo, hi = piece
        klass = cls[s * SLAB : (s + 1) * SLAB, lo:hi]
        value = jnp.full(klass.shape, table[0, 0], jnp.float32)
        for k in range(1, table.shape[1]):
            value = jnp.where(klass == k, table[0, k], value)
        cond[PAD + s * SLAB : PAD + (s + 1) * SLAB, lo:hi] = value

    for b in range(1, len(blocks)):
        load_class(b).wait()
    for piece in rim:
        lookup(piece)
    pl.semaphore_wait(barrier, greeted)
    send_borders(0, cond)
    load_class(0).wait()
    for piece in middle:
        lookup(piece)
    for load in loads:
        load.wait()

    def setup(piece):
        s, lo, hi = piece
        at = slice(s * SLAB, (s + 1) * SLAB)
        here, beside = around(cond, piece)
        diagonal = via_conductance * via[at, lo:hi].astype(jnp.float32)
        diagonal = diagonal + pad_conductance * pad[at, lo:hi].astype(jnp.float32) + leakage
        for k in range(4):
            value = jnp.where(beside[k] > 0.0, 0.5 * (here + beside[k]), 0.0)
            edge[k, at, lo:hi] = value
            diagonal = diagonal + value
        recip = 1.0 / diagonal
        inv[at, lo:hi] = recip
        zed[PAD + s * SLAB : PAD + (s + 1) * SLAB, lo:hi] = cur[at, lo:hi] * recip

    def image(field, other, base, piece):
        s, lo, hi = piece
        at = slice(s * SLAB, (s + 1) * SLAB)
        here, beside = around(field, piece)
        total = edge[0, at, lo:hi] * beside[0] + edge[1, at, lo:hi] * beside[1]
        total = total + (edge[2, at, lo:hi] * beside[2] + edge[3, at, lo:hi] * beside[3])
        cross = via_conductance * via[at, lo:hi].astype(jnp.float32) * other[at, lo:hi]
        return here, base - total - cross

    def ahead(sums, piece):
        s, lo, hi = piece
        at = slice(s * SLAB, (s + 1) * SLAB)
        base = cur[at, lo:hi]
        here, w = image(zed, zedq, base, piece)
        y = w * inv[at, lo:hi]
        wed[at, lo:hi] = w
        yed[PAD + s * SLAB : PAD + (s + 1) * SLAB, lo:hi] = y
        terms = (base * here, w * here, w * y)
        return tuple(total + fold(term) for total, term in zip(sums, terms))

    def depart(rnd, field):
        send_borders(rnd + 1, field)
        for b in range(1, len(blocks)):
            to_partner(rnd, b).start()

    def meanwhile(rnd, work, sums):
        to_partner(rnd, 0).wait_recv()
        for piece in middle:
            sums = work(sums, piece)
        return sums

    def arrive(rnd, field, work, sums):
        take_borders(rnd + 1, field)
        for b in range(1, len(blocks)):
            to_partner(rnd, b).wait_recv()
        for piece in rim:
            sums = work(sums, piece)
        return sums

    for piece in middle:
        setup(piece)
    to_partner(0, 0).start()
    take_borders(0, cond)
    for piece in rim:
        setup(piece)

    nothing = jnp.zeros((SLAB, 128), jnp.float32)
    depart(0, zed)
    sums = meanwhile(0, ahead, (nothing,) * 3)
    to_partner(1, 0).start()
    gamma, delta, eps = arrive(0, zed, ahead, sums)
    depart(1, yed)

    eps_all = jnp.sum(eps, keepdims=True)
    delta_all = jnp.sum(delta, keepdims=True)
    a_d = jnp.where(eps_all > 0.0, delta_all / jnp.where(eps_all > 0.0, eps_all, 1.0), 0.0)

    def again(sums, piece):
        s, lo, hi = piece
        at = slice(s * SLAB, (s + 1) * SLAB)
        w = wed[at, lo:hi]
        y, u = image(yed, yedq, w, piece)
        ued[at, lo:hi] = u
        r1 = cur[at, lo:hi] - a_d * w
        z1 = zed[PAD + s * SLAB : PAD + (s + 1) * SLAB, lo:hi] - a_d * y
        w1 = w - a_d * u
        terms = (r1 * z1, w * z1, z1 * w1, z1 * u + y * w1, y * u)
        return tuple(total + fold(term) for total, term in zip(sums, terms))

    sums = meanwhile(1, again, (nothing,) * 5)
    s0, s1, t0, t1, t2 = arrive(1, yed, again, sums)

    packet = jnp.zeros((SLAB, 128), jnp.float32)
    for k, value in enumerate((gamma, delta, s0, s1, eps, t0, t1, t2)):
        packet = packet + jnp.where(lane == k, jnp.sum(value, axis=1, keepdims=True), 0.0)
    packet = jnp.sum(packet, axis=0, keepdims=True)
    packet = jnp.where(lane[0:1] == 8, a_d, packet)
    gather[0] = packet

    def share(k):
        return pltpu.make_async_remote_copy(
            src_ref=gather.at[0], dst_ref=gather.at[k], send_sem=sum_send, recv_sem=sum_recv,
            device_id=peer(k), device_id_type=MESH)

    each_peer(lambda k: share(k).start())
    everyone = gather.at[pl.ds(1, others)]
    pltpu.make_async_copy(everyone, everyone, sum_recv).wait()

    table_in = gather[...].reshape(others + 1, 128)
    lanes = lax.broadcasted_iota(jnp.int32, table_in.shape, 1)
    g, d, s0, s1, s2, t0, t1, t2, a_ds = (
        jnp.sum(jnp.where(lanes == k, table_in, 0.0), axis=1, keepdims=True) for k in range(9)
    )
    energy = jnp.sum(g, axis=0, keepdims=True)
    step = energy / jnp.sum(d, axis=0, keepdims=True)
    away = step - a_ds
    energy_next = jnp.sum(s0 - 2.0 * away * s1 + away * away * s2, axis=0, keepdims=True)
    curve = jnp.sum(t0 - away * t1 + away * away * t2, axis=0, keepdims=True)
    ratio = energy_next / energy
    step_next = energy_next / (curve - ratio * energy_next / step)

    for k, value in enumerate((step, step_next, ratio)):
        scal[k : k + 1, :] = jnp.broadcast_to(value, (1, 128))

    for rnd in range(3):
        for way in range(4):
            if exists[way]:
                pl.when(present[way])(lambda rnd=rnd, way=way: border(rnd, way).wait_send())
    for rnd in range(2):
        for b in range(len(blocks)):
            to_partner(rnd, b).wait_send()
    pltpu.make_async_copy(everyone, everyone, sum_send).wait()


def finish(cur, zed, wed, yed, ued, scal, drop_hbm, res_hbm, worst_hbm, out, store_sem):
    height = cur.shape[0]
    slabs = height // SLAB
    chunks = store_sem.shape[1]
    chunk = height // chunks
    step, step_next, ratio = (scal[k : k + 1, 0:1] for k in range(3))
    stores = []
    for s in range(slabs):
        at = slice(s * SLAB, (s + 1) * SLAB)
        z = zed[PAD + s * SLAB : PAD + (s + 1) * SLAB, :]
        y = yed[PAD + s * SLAB : PAD + (s + 1) * SLAB, :]
        w = wed[at, :]
        first = step * z
        drop = first + step_next * ((z - step * y) + ratio * z)
        out[0, at, :] = drop
        out[1, at, :] = (cur[at, :] - step * w) - step_next * ((w - step * ued[at, :]) + ratio * w)
        out[2, at, :] = jnp.maximum(first, drop)
        if (s + 1) * SLAB % chunk == 0:
            c = (s + 1) * SLAB // chunk - 1
            for k, dst in enumerate((drop_hbm, res_hbm, worst_hbm)):
                store = pltpu.make_async_copy(
                    out.at[k, pl.ds(c * chunk, chunk)], dst.at[0, pl.ds(c * chunk, chunk)],
                    store_sem.at[k, c])
                store.start()
                stores.append(store)

    for store in stores:
        store.wait()


def local(sizes, current, node_class, class_conductance, pad_mask, via_mask):
    _, height, width = current.shape
    f32 = jnp.float32
    chunks = 8
    full = lambda kind=f32: pltpu.VMEM((height, width), kind)
    tall = pltpu.VMEM((height + 2 * PAD, width), f32)
    anywhere = pl.BlockSpec(memory_space=pl.ANY)
    dma = pltpu.SemaphoreType.DMA
    kept = [(height, width), tall.shape, (height, width), tall.shape, (height, width), (8, 128)]
    far = pl.BlockSpec(memory_space=pltpu.HBM)
    inside = pl.BlockSpec(memory_space=pltpu.VMEM)
    fields = pl.pallas_call(
        functools.partial(kernel, sizes),
        out_shape=[pltpu.VMEM(shape, f32) for shape in kept],
        in_specs=[far, far, pl.BlockSpec(memory_space=pltpu.SMEM), far, far],
        out_specs=[inside] * len(kept),
        scratch_shapes=[
            full(jnp.int32), full(jnp.int32), full(jnp.int32),
            tall, pltpu.VMEM((4, height, width), f32), full(), full(), full(),
            pltpu.VMEM((3, 2, 1, width), f32), pltpu.VMEM((3, 2, 1, width), f32),
            pltpu.VMEM((3, 2, 1, height), f32), pltpu.VMEM((3, 2, 1, height), f32),
            pltpu.VMEM((2, height, 128), f32),
            pltpu.VMEM((sizes[0] * sizes[1] * sizes[2], 1, 128), f32),
            dma((8,)), dma((3, 4)), dma((3, 4)), dma((2, 5)), dma((2, 5)), dma, dma,
        ],
        compiler_params=pltpu.CompilerParams(
            collective_id=0, has_side_effects=True, vmem_limit_bytes=56 * 2**20),
    )(current, node_class, class_conductance, pad_mask, via_mask)
    return pl.pallas_call(
        finish,
        out_shape=[jax.ShapeDtypeStruct(current.shape, f32)] * 3,
        in_specs=[inside] * len(kept),
        out_specs=[anywhere] * 3,
        scratch_shapes=[pltpu.VMEM((3, height, width), f32), dma((3, chunks))],
        compiler_params=pltpu.CompilerParams(vmem_limit_bytes=8 * 2**20),
    )(*fields)


def solution(mesh):
    field = P("layer", ("scen", "row"), "col")
    sizes = tuple(mesh.shape[name] for name in ("row", "col", "layer"))
    return jax.shard_map(
        functools.partial(local, sizes),
        mesh=mesh,
        in_specs=(field, field, P("layer", None), field, P(("scen", "row"), "col")),
        out_specs=(field, field, field),
        check_vma=False,
    )
```

```python
import functools

import jax
import jax.numpy as jnp
from jax import lax
from jax.experimental import pallas as pl
from jax.experimental.pallas import tpu as pltpu
from jax.sharding import PartitionSpec as P

MESH = pl.DeviceIdType.MESH
PAD = 8
SLAB = 8
via_conductance = 2.0
pad_conductance = 4.0
leakage = 0.05


def fold(x):
    parts = [x[:, k : k + 128] for k in range(0, x.shape[1], 128)]
    while len(parts) > 1:
        half = len(parts) // 2
        parts = [parts[k] + parts[k + half] for k in range(half)] + parts[2 * half :]
    return parts[0]


def kernel(sizes, cur_hbm, cls_hbm, table, pad_hbm, via_hbm, cur, zed, wed, yed, ued, scal,
           cls, pad, via, cond, edge, inv, zedq, yedq,
           row_out, row_in, col_out, col_in, side, gather,
           load_sem, edge_send, edge_recv, layer_send, layer_recv, sum_send, sum_recv):
    rows, cols, layers = sizes
    height, width = cur.shape
    me_r, me_c, me_l = lax.axis_index("row"), lax.axis_index("col"), lax.axis_index("layer")
    others = rows * cols * layers - 1
    slabs = height // SLAB

    def peer(k):
        r = lax.rem(me_r + k // (cols * layers), rows)
        c = lax.rem(me_c + lax.rem(k // layers, cols), cols)
        l = lax.rem(me_l + lax.rem(k, layers), layers)
        return {"row": r, "col": c, "layer": l}

    def each_peer(body):
        if others < 32:
            for k in range(1, others + 1):
                body(k)
        else:
            def step(k, carry):
                body(k)
                return carry
            lax.fori_loop(1, others + 1, step, 0)

    inner = (128, width - 128)
    middle = [(s, *inner) for s in range(1, slabs - 1)]
    rim = [(0, 0, width), (slabs - 1, 0, width)]
    rim += [(s, lo, hi) for s in range(1, slabs - 1) for lo, hi in ((0, 128), (width - 128, width))]

    blocks = (
        (SLAB, height - SLAB, *inner),
        (0, SLAB, 0, width), (height - SLAB, height, 0, width),
        (SLAB, height - SLAB, 0, 128), (SLAB, height - SLAB, width - 128, width),
    )

    def load_class(b):
        top, bottom, lo, hi = blocks[b]
        return pltpu.make_async_copy(
            cls_hbm.at[0, pl.ds(top, bottom - top), pl.ds(lo, hi - lo)],
            cls.at[pl.ds(top, bottom - top), pl.ds(lo, hi - lo)], load_sem.at[3 + b])

    loads = [
        pltpu.make_async_copy(src, dst, load_sem.at[k])
        for k, (src, dst) in enumerate(
            ((via_hbm, via), (pad_hbm.at[0], pad), (cur_hbm.at[0], cur)))
    ]
    for b in (1, 2, 3, 4, 0):
        load_class(b).start()
    barrier = pltpu.get_barrier_semaphore()
    def greet(k):
        pl.semaphore_signal(barrier, inc=1, device_id=peer(k), device_id_type=MESH)

    if rows + cols <= 6:
        for k in range(1, layers):
            greet(k)
        greeted = layers - 1
        near = (
            ("row", me_r - 1, me_r > 0), ("row", me_r + 1, me_r < rows - 1),
            ("col", me_c - 1, me_c > 0), ("col", me_c + 1, me_c < cols - 1),
        )
        for axis, there, is_there in near:
            def beyond(axis=axis, there=there):
                for k in range(layers):
                    l = lax.rem(me_l + k, layers)
                    pl.semaphore_signal(barrier, inc=1, device_id={axis: there, "layer": l},
                                        device_id_type=MESH)
            if (rows if axis == "row" else cols) > 1:
                pl.when(is_there)(beyond)
                greeted = greeted + layers * is_there.astype(jnp.int32)
    else:
        each_peer(greet)
        greeted = others

    for load in loads:
        load.start()

    present = (me_r > 0, me_r < rows - 1, me_c > 0, me_c < cols - 1)
    exists = (rows > 1, rows > 1, cols > 1, cols > 1)
    target = ({"row": me_r - 1}, {"row": me_r + 1}, {"col": me_c - 1}, {"col": me_c + 1})

    def border(rnd, way):
        src = row_out if way < 2 else col_out
        dst = row_in if way < 2 else col_in
        return pltpu.make_async_remote_copy(
            src_ref=src.at[rnd, way % 2],
            dst_ref=dst.at[rnd, 1 - way % 2],
            send_sem=edge_send.at[rnd, way],
            recv_sem=edge_recv.at[rnd, way ^ 1],
            device_id=target[way],
            device_id_type=MESH,
        )

    def arrival(rnd, way):
        buf = row_in if way < 2 else col_in
        return pltpu.make_async_copy(
            buf.at[rnd, way % 2], buf.at[rnd, way % 2], edge_recv.at[rnd, way]
        )

    def send_borders(rnd, field):
        row_out[rnd, 0] = field[PAD : PAD + 1, :]
        row_out[rnd, 1] = field[PAD + height - 1 : PAD + height, :]
        for way in (0, 1):
            if exists[way]:
                pl.when(present[way])(lambda way=way: border(rnd, way).start())
        for way, lo, lane_at in ((2, 0, 0), (3, width - 128, 127)):
            def turn(way=way, lo=lo, lane_at=lane_at):
                column = jnp.transpose(field[PAD : PAD + height, lo : lo + 128])
                col_out[rnd, way - 2] = column[lane_at : lane_at + 1, :]
                border(rnd, way).start()
            if exists[way]:
                pl.when(present[way])(turn)

    def take_borders(rnd, field):
        for way in range(4):
            if exists[way]:
                pl.when(present[way])(lambda way=way: arrival(rnd, way).wait())
        field[PAD - 1 : PAD, :] = row_in[rnd, 0]
        field[PAD + height : PAD + height + 1, :] = row_in[rnd, 1]
        for k in range(2):
            def turn(k=k):
                side[k] = jnp.transpose(jnp.broadcast_to(col_in[rnd, k], (128, height)))
            if exists[2 + k]:
                pl.when(present[2 + k])(turn)

    def clear(rnd):
        for way in range(4):
            buf = row_in if way < 2 else col_in
            def zero(buf=buf, way=way):
                buf[rnd, way % 2] = jnp.zeros(buf.shape[2:], jnp.float32)
            if exists[way]:
                pl.when(jnp.logical_not(present[way]))(zero)
            else:
                zero()

    for rnd in range(3):
        clear(rnd)
    for k in range(2):
        side[k] = jnp.zeros(side.shape[1:], jnp.float32)

    lane = lax.broadcasted_iota(jnp.int32, (SLAB, 128), 1)

    def around(field, piece):
        s, lo, hi = piece
        top = PAD + s * SLAB
        at = slice(s * SLAB, (s + 1) * SLAB)
        north = field[top - 1 : top + SLAB - 1, lo:hi]
        south = field[top + 1 : top + SLAB + 1, lo:hi]
        first, last = max(lo - 128, 0), min(hi + 128, width)
        wide = field[top : top + SLAB, first:last]
        here = wide[:, lo - first : hi - first]
        west = pltpu.roll(wide, 1, 1)[:, lo - first : hi - first]
        east = pltpu.roll(wide, last - first - 1, 1)[:, lo - first : hi - first]
        if lo == 0:
            edge_tile = jnp.where(lane == 0, side[0, at, :], west[:, :128])
            west = edge_tile if hi == 128 else jnp.concatenate([edge_tile, west[:, 128:]], axis=1)
        if hi == width:
            edge_tile = jnp.where(lane == 127, side[1, at, :], east[:, -128:])
            east = edge_tile if hi - lo == 128 else jnp.concatenate([east[:, :-128], edge_tile], axis=1)
        return here, (north, south, west, east)

    def to_partner(rnd, b):
        top, bottom, lo, hi = blocks[b]
        src = (zed, yed)[rnd].at[pl.ds(PAD + top, bottom - top), pl.ds(lo, hi - lo)]
        dst = (zedq, yedq)[rnd].at[pl.ds(top, bottom - top), pl.ds(lo, hi - lo)]
        return pltpu.make_async_remote_copy(
            src_ref=src, dst_ref=dst,
            send_sem=layer_send.at[rnd, b], recv_sem=layer_recv.at[rnd, b],
            device_id={"layer": 1 - me_l}, device_id_type=MESH)

    def lookup(piece):
        s, lo, hi = piece
        klass = cls[s * SLAB : (s + 1) * SLAB, lo:hi]
        value = jnp.full(klass.shape, table[0, 0], jnp.float32)
        for k in range(1, table.shape[1]):
            value = jnp.where(klass == k, table[0, k], value)
        cond[PAD + s * SLAB : PAD + (s + 1) * SLAB, lo:hi] = value

    for b in range(1, len(blocks)):
        load_class(b).wait()
    for piece in rim:
        lookup(piece)
    pl.semaphore_wait(barrier, greeted)
    send_borders(0, cond)
    load_class(0).wait()
    for piece in middle:
        lookup(piece)
    for load in loads:
        load.wait()

    def setup(piece):
        s, lo, hi = piece
        at = slice(s * SLAB, (s + 1) * SLAB)
        here, beside = around(cond, piece)
        diagonal = via_conductance * via[at, lo:hi].astype(jnp.float32)
        diagonal = diagonal + pad_conductance * pad[at, lo:hi].astype(jnp.float32) + leakage
        for k in range(4):
            value = jnp.where(beside[k] > 0.0, 0.5 * (here + beside[k]), 0.0)
            edge[k, at, lo:hi] = value
            diagonal = diagonal + value
        recip = 1.0 / diagonal
        inv[at, lo:hi] = recip
        zed[PAD + s * SLAB : PAD + (s + 1) * SLAB, lo:hi] = cur[at, lo:hi] * recip

    def image(field, other, base, piece):
        s, lo, hi = piece
        at = slice(s * SLAB, (s + 1) * SLAB)
        here, beside = around(field, piece)
        total = edge[0, at, lo:hi] * beside[0] + edge[1, at, lo:hi] * beside[1]
        total = total + (edge[2, at, lo:hi] * beside[2] + edge[3, at, lo:hi] * beside[3])
        cross = via_conductance * via[at, lo:hi].astype(jnp.float32) * other[at, lo:hi]
        return here, base - total - cross

    def ahead(sums, piece):
        s, lo, hi = piece
        at = slice(s * SLAB, (s + 1) * SLAB)
        base = cur[at, lo:hi]
        here, w = image(zed, zedq, base, piece)
        y = w * inv[at, lo:hi]
        wed[at, lo:hi] = w
        yed[PAD + s * SLAB : PAD + (s + 1) * SLAB, lo:hi] = y
        terms = (base * here, w * here, w * y)
        return tuple(total + fold(term) for total, term in zip(sums, terms))

    def depart(rnd, field):
        send_borders(rnd + 1, field)
        for b in range(1, len(blocks)):
            to_partner(rnd, b).start()

    def meanwhile(rnd, work, sums):
        to_partner(rnd, 0).wait_recv()
        for piece in middle:
            sums = work(sums, piece)
        return sums

    def arrive(rnd, field, work, sums):
        take_borders(rnd + 1, field)
        for b in range(1, len(blocks)):
            to_partner(rnd, b).wait_recv()
        for piece in rim:
            sums = work(sums, piece)
        return sums

    for piece in middle:
        setup(piece)
    to_partner(0, 0).start()
    take_borders(0, cond)
    for piece in rim:
        setup(piece)

    nothing = jnp.zeros((SLAB, 128), jnp.float32)
    depart(0, zed)
    sums = meanwhile(0, ahead, (nothing,) * 3)
    to_partner(1, 0).start()
    gamma, delta, eps = arrive(0, zed, ahead, sums)
    depart(1, yed)

    eps_all = jnp.sum(eps, keepdims=True)
    delta_all = jnp.sum(delta, keepdims=True)
    a_d = jnp.where(eps_all > 0.0, delta_all / jnp.where(eps_all > 0.0, eps_all, 1.0), 0.0)

    def again(sums, piece):
        s, lo, hi = piece
        at = slice(s * SLAB, (s + 1) * SLAB)
        w = wed[at, lo:hi]
        y, u = image(yed, yedq, w, piece)
        ued[at, lo:hi] = u
        r1 = cur[at, lo:hi] - a_d * w
        z1 = zed[PAD + s * SLAB : PAD + (s + 1) * SLAB, lo:hi] - a_d * y
        w1 = w - a_d * u
        terms = (r1 * z1, w * z1, z1 * w1, z1 * u + y * w1, y * u)
        return tuple(total + fold(term) for total, term in zip(sums, terms))

    sums = meanwhile(1, again, (nothing,) * 5)
    s0, s1, t0, t1, t2 = arrive(1, yed, again, sums)

    packet = jnp.zeros((SLAB, 128), jnp.float32)
    for k, value in enumerate((gamma, delta, s0, s1, eps, t0, t1, t2)):
        packet = packet + jnp.where(lane == k, jnp.sum(value, axis=1, keepdims=True), 0.0)
    packet = jnp.sum(packet, axis=0, keepdims=True)
    packet = jnp.where(lane[0:1] == 8, a_d, packet)
    gather[0] = packet

    def share(k):
        return pltpu.make_async_remote_copy(
            src_ref=gather.at[0], dst_ref=gather.at[k], send_sem=sum_send, recv_sem=sum_recv,
            device_id=peer(k), device_id_type=MESH)

    each_peer(lambda k: share(k).start())
    everyone = gather.at[pl.ds(1, others)]
    pltpu.make_async_copy(everyone, everyone, sum_recv).wait()

    table_in = gather[...].reshape(others + 1, 128)
    lanes = lax.broadcasted_iota(jnp.int32, table_in.shape, 1)
    g, d, s0, s1, s2, t0, t1, t2, a_ds = (
        jnp.sum(jnp.where(lanes == k, table_in, 0.0), axis=1, keepdims=True) for k in range(9)
    )
    energy = jnp.sum(g, axis=0, keepdims=True)
    step = energy / jnp.sum(d, axis=0, keepdims=True)
    away = step - a_ds
    energy_next = jnp.sum(s0 - 2.0 * away * s1 + away * away * s2, axis=0, keepdims=True)
    curve = jnp.sum(t0 - away * t1 + away * away * t2, axis=0, keepdims=True)
    ratio = energy_next / energy
    step_next = energy_next / (curve - ratio * energy_next / step)

    for k, value in enumerate((step, step_next, ratio)):
        scal[k : k + 1, :] = jnp.broadcast_to(value, (1, 128))

    for rnd in range(3):
        for way in range(4):
            if exists[way]:
                pl.when(present[way])(lambda rnd=rnd, way=way: border(rnd, way).wait_send())
    for rnd in range(2):
        for b in range(len(blocks)):
            to_partner(rnd, b).wait_send()
    pltpu.make_async_copy(everyone, everyone, sum_send).wait()


def finish(cur, zed, wed, yed, ued, scal, drop_hbm, res_hbm, worst_hbm, out, store_sem):
    height = cur.shape[0]
    slabs = height // SLAB
    chunks = store_sem.shape[1]
    chunk = height // chunks
    step, step_next, ratio = (scal[k : k + 1, 0:1] for k in range(3))
    stores = []
    for s in range(slabs):
        at = slice(s * SLAB, (s + 1) * SLAB)
        z = zed[PAD + s * SLAB : PAD + (s + 1) * SLAB, :]
        y = yed[PAD + s * SLAB : PAD + (s + 1) * SLAB, :]
        w = wed[at, :]
        first = step * z
        drop = first + step_next * ((z - step * y) + ratio * z)
        out[0, at, :] = drop
        out[1, at, :] = (cur[at, :] - step * w) - step_next * ((w - step * ued[at, :]) + ratio * w)
        out[2, at, :] = jnp.maximum(first, drop)
        if (s + 1) * SLAB % chunk == 0:
            c = (s + 1) * SLAB // chunk - 1
            for k, dst in enumerate((drop_hbm, res_hbm, worst_hbm)):
                store = pltpu.make_async_copy(
                    out.at[k, pl.ds(c * chunk, chunk)], dst.at[0, pl.ds(c * chunk, chunk)],
                    store_sem.at[k, c])
                store.start()
                stores.append(store)

    for store in stores:
        store.wait()


def local(sizes, current, node_class, class_conductance, pad_mask, via_mask):
    _, height, width = current.shape
    f32 = jnp.float32
    chunks = 4
    full = lambda kind=f32: pltpu.VMEM((height, width), kind)
    tall = pltpu.VMEM((height + 2 * PAD, width), f32)
    anywhere = pl.BlockSpec(memory_space=pl.ANY)
    dma = pltpu.SemaphoreType.DMA
    kept = [(height, width), tall.shape, (height, width), tall.shape, (height, width), (8, 128)]
    far = pl.BlockSpec(memory_space=pltpu.HBM)
    inside = pl.BlockSpec(memory_space=pltpu.VMEM)
    fields = pl.pallas_call(
        functools.partial(kernel, sizes),
        out_shape=[pltpu.VMEM(shape, f32) for shape in kept],
        in_specs=[far, far, pl.BlockSpec(memory_space=pltpu.SMEM), far, far],
        out_specs=[inside] * len(kept),
        scratch_shapes=[
            full(jnp.int32), full(jnp.int32), full(jnp.int32),
            tall, pltpu.VMEM((4, height, width), f32), full(), full(), full(),
            pltpu.VMEM((3, 2, 1, width), f32), pltpu.VMEM((3, 2, 1, width), f32),
            pltpu.VMEM((3, 2, 1, height), f32), pltpu.VMEM((3, 2, 1, height), f32),
            pltpu.VMEM((2, height, 128), f32),
            pltpu.VMEM((sizes[0] * sizes[1] * sizes[2], 1, 128), f32),
            dma((8,)), dma((3, 4)), dma((3, 4)), dma((2, 5)), dma((2, 5)), dma, dma,
        ],
        compiler_params=pltpu.CompilerParams(
            collective_id=0, has_side_effects=True, vmem_limit_bytes=56 * 2**20),
    )(current, node_class, class_conductance, pad_mask, via_mask)
    return pl.pallas_call(
        finish,
        out_shape=[jax.ShapeDtypeStruct(current.shape, f32)] * 3,
        in_specs=[inside] * len(kept),
        out_specs=[anywhere] * 3,
        scratch_shapes=[pltpu.VMEM((3, height, width), f32), dma((3, chunks))],
        compiler_params=pltpu.CompilerParams(vmem_limit_bytes=8 * 2**20),
    )(*fields)


def solution(mesh):
    field = P("layer", ("scen", "row"), "col")
    sizes = tuple(mesh.shape[name] for name in ("row", "col", "layer"))
    return jax.shard_map(
        functools.partial(local, sizes),
        mesh=mesh,
        in_specs=(field, field, P("layer", None), field, P(("scen", "row"), "col")),
        out_specs=(field, field, field),
        check_vma=False,
    )
```
